256 devices in a mesh: grp: 8 (over y, z_hi), dev: 32 (over x, z_lo, core).
Axes of the slice: x: 4, y: 4, z: 8 (z_hi: 2, z_lo: 4; z = z_hi * 4 + z_lo), core: 2. Of those that a mesh axis runs over, the one named last changes fastest.
Arguments:
- sources: bfloat16 [524288, 768], P(('grp', 'dev')), may hold values from -6 to 6
- encoder: bfloat16 [524288, 256], P(('grp', 'dev')), may hold values from -0.125 to 0.125
- section_weight: bfloat16 [256, 5, 2, 256, 256], P(('grp', 'dev')), may hold values from -0.25 to 0.25
- cross_weight: bfloat16 [8, 32, 8, 256, 256], P('grp', 'dev'), may hold values from -0.125 to 0.125
- local_weight: bfloat16 [256, 14, 256, 256], P(('grp', 'dev')), may hold values from -0.375 to 0.375
- decoder: bfloat16 [524288, 256], P(('grp', 'dev')), may hold values from -0.375 to 0.375
Outputs:
- target_values: bfloat16 [524288, 768], P(('grp', 'dev'))
The draws below stay inside these ranges and needn't reach their ends.
All inputs are finite; a program needn't handle non-finite values.
Results may differ from the reference program's by a relative error of at most 0.02.
Values may be sent and summed in bfloat16 or wider, within the bound.
A program may use at most 64 MiB of HBM per device.

```python
import jax
import jax.numpy as jnp
import numpy as np

K = 256
R = 768
PTS_DEV = 2048
LOCAL = 3
BITS = 5
MATS = 14
LEAF_T = 256
NPTS = 524288
N_GRP = 8
N_DEV = 32


def shard_levels(key, shape, shards, smallest, high):
    factor_of = 1.0
    for dim, parts in shards:
        steps = jax.random.uniform(jax.random.fold_in(jax.random.fold_in(key, 6), dim), (parts,), jnp.float32, smallest / len(shards), high / len(shards))
        factor_of = factor_of * jnp.repeat(jnp.exp(steps), shape[dim] // parts).reshape((-1,) + (1,) * (len(shape) - 1 - dim))
    return factor_of


def scatter_about(stream_key, dims, spread, most, shards=(), kind=jnp.bfloat16):
    array = spread * jax.random.normal(stream_key, dims, jnp.float32)
    if shards:
        array = array * shard_levels(stream_key, dims, shards, -0.22, 0.18)
    return jnp.clip(array, -most, most).astype(kind)


def setup_inputs(seed: int = 0) -> dict:
    streams_of = jax.random.split(jax.random.key(seed), 7)
    sources = scatter_about(streams_of[0], (NPTS, R), 1.0, 6.0, ((0, 256),))
    encoder = scatter_about(streams_of[1], (NPTS, K), PTS_DEV ** -0.5, 0.125, ((0, 256),))
    section_weight = scatter_about(streams_of[2], (N_GRP * N_DEV, BITS, 2, K, K), (2 * K) ** -0.5, 0.25, ((0, 256),))
    cross_weight = scatter_about(streams_of[3], (N_GRP, N_DEV, N_GRP, K, K), (N_GRP * K) ** -0.5, 0.125, ((0, 8), (1, 32)))
    local_weight = scatter_about(streams_of[4], (N_GRP * N_DEV, MATS, K, K), K ** -0.5, 0.375, ((0, 256),))
    decoder = scatter_about(streams_of[5], (NPTS, K), K ** -0.5, 0.375, ((0, 256),))
    return dict(sources=sources, encoder=encoder, section_weight=section_weight, cross_weight=cross_weight, local_weight=local_weight, decoder=decoder)


def reference(sources, encoder, section_weight, cross_weight, local_weight, decoder):
    devices_all = N_GRP * N_DEV
    source_rows = sources.reshape(devices_all, PTS_DEV, R).astype(jnp.float32)
    encoder_rows = encoder.reshape(devices_all, PTS_DEV, K).astype(jnp.float32)
    coeffs = jnp.einsum('pnk,pnr->pkr', encoder_rows, source_rows).astype(jnp.bfloat16)
    for section_bit in range(BITS):
        partner = np.arange(devices_all) ^ (1 << section_bit)
        partner_coeffs = coeffs[partner]
        matrices = section_weight[:, section_bit].astype(jnp.float32)
        coeffs = (jnp.einsum('pkl,plr->pkr', matrices[:, 0], coeffs.astype(jnp.float32))
                  + jnp.einsum('pkl,plr->pkr', matrices[:, 1], partner_coeffs.astype(jnp.float32))).astype(jnp.bfloat16)
    grouped = coeffs.reshape(N_GRP, N_DEV, K, R).astype(jnp.float32)
    merged = jnp.einsum('gdhkl,hdlr->gdkr', cross_weight.astype(jnp.float32), grouped).astype(jnp.bfloat16)
    blocks = merged.reshape(devices_all, 1, K, R)
    offset = 0
    for depth_level in range(LOCAL):
        children = 2 ** (depth_level + 1)
        matrices = local_weight[:, offset:offset + children].astype(jnp.float32)
        matrices = matrices.reshape(devices_all, children // 2, 2, K, K)
        blocks = jnp.einsum('pjckl,pjlr->pjckr', matrices, blocks.astype(jnp.float32))
        blocks = blocks.reshape(devices_all, children, K, R).astype(jnp.bfloat16)
        offset = offset + children
    decoder_leaves = decoder.reshape(devices_all, 2 ** LOCAL, LEAF_T, K).astype(jnp.float32)
    target_values = jnp.einsum('pctk,pckr->pctr', decoder_leaves, blocks.astype(jnp.float32))
    return target_values.reshape(NPTS, R).astype(jnp.bfloat16)
```

```python
import math

import jax
import jax.numpy as jnp
from jax import lax
from jax.experimental import pallas as pl
from jax.experimental.pallas import tpu as pltpu
from jax.sharding import PartitionSpec as P

K = 256
LOCAL = 3
SECTIONS = 5
GROUPS = 8
WIDTH = 128
MESH = pl.DeviceIdType.MESH

TIMES = {
    "encode": 0.0,
    "section0": 0.45,
    "section1": 1.6,
    "section2": 3.4,
    "section3": 4.5,
    "section4": 5.7,
    "relay": 6.8,
    "spread": 8.2,
    "relay_far": 9.3,
    "finish": 10.3,
}

OWN, BELOW, ABOVE, ACROSS, FAR, FAR_BELOW, FAR_ABOVE, FAR_ACROSS = range(GROUPS)
(TO_BELOW, TO_ABOVE, TO_ACROSS_UP, TO_ACROSS_DOWN, TO_FAR,
 TO_FAR_BELOW, TO_FAR_ABOVE, TO_FAR_ACROSS_UP, TO_FAR_ACROSS_DOWN) = range(SECTIONS, SECTIONS + 9)
COPIES = SECTIONS + 9


def flip(index, bit):
    size = 2**bit
    return index + size - 2 * size * lax.rem(lax.div(index, size), 2)


def kernel(sources, encoder, section_weight, cross_weight, local_weight, decoder, target,
           src, enc, enc_t, pair_w, cross_w, local_w, dec, pairs, gathered, blocks, out,
           load_sem, src_sem, out_sem, send_sem, recv_sem):
    chunks = src.shape[0]
    grp, dev = lax.axis_index("grp"), lax.axis_index("dev")
    height = lax.div(grp, 2)
    half = lax.rem(grp, 2)

    def group(step, far):
        return 2 * lax.rem(height + step, 4) + (1 - half if far else half)

    partners = [(grp, flip(dev, bit)) for bit in range(SECTIONS)]
    below, above, far = (group(3, False), dev), (group(1, False), dev), (group(0, True), dev)

    barrier = pltpu.get_barrier_semaphore()
    for device in (*partners, below, above, far):
        pl.semaphore_signal(barrier, inc=1, device_id=device, device_id_type=MESH)

    def load_sources(j):
        return pltpu.make_async_copy(
            sources.at[:, pl.ds(pl.multiple_of(j * WIDTH, WIDTH), WIDTH)], src.at[j], src_sem.at[j]
        )

    loads = {"encoder": [(encoder, enc)]}
    for bit in range(SECTIONS):
        loads[f"section{bit}"] = [
            (section_weight.at[0, bit, side], pair_w.at[bit, :, pl.ds(side * K, K)]) for side in range(2)
        ]
    order = [group(step, away) for away in (False, True) for step in (0, 3, 1, 2)]
    loads["cross"] = [
        (cross_weight.at[0, 0, order[slot]], cross_w.at[:, pl.ds(slot * K, K)]) for slot in range(GROUPS)
    ]
    loads["local"] = [(local_weight.at[0], local_w)]
    loads["decoder"] = [(decoder, dec)]
    copies, number = {}, 0
    for name, moves in loads.items():
        copies[name] = []
        for start, end in moves:
            copies[name].append(pltpu.make_async_copy(start, end, load_sem.at[number]))
            number += 1

    def begin(name):
        for copy in copies[name]:
            copy.start()

    def ready(name):
        for copy in copies[name]:
            copy.wait()

    begin("encoder")
    load_sources(0).start()
    begin("section0")
    for j in range(1, chunks):
        load_sources(j).start()
    for bit in range(1, SECTIONS):
        begin(f"section{bit}")
    begin("cross")
    begin("local")
    begin("decoder")

    ready("encoder")
    for block in range(enc.shape[0] // K):
        rows = pl.ds(block * K, K)
        enc_t[:, rows] = enc[rows, :].T
    pl.semaphore_wait(barrier, 8)

    def copy(kind, j, start, end, device):
        return pltpu.make_async_remote_copy(
            src_ref=start, dst_ref=end, send_sem=send_sem.at[kind, j], recv_sem=recv_sem.at[kind, j],
            device_id=device, device_id_type=MESH,
        )

    def slot(j, number, first=0, rows=K):
        return gathered.at[j, pl.ds(number * K + first, rows)]

    def exchange(bit, j):
        return copy(bit, j, pairs.at[bit, j, pl.ds(0, K)], pairs.at[bit, j, pl.ds(K, K)], partners[bit])

    def gather(kind, j):
        upper, lower = (0, K // 2), (K // 2, K // 2)
        start, end, device = {
            TO_ABOVE: (slot(j, OWN), slot(j, BELOW), above),
            TO_BELOW: (slot(j, OWN), slot(j, ABOVE), below),
            TO_ACROSS_UP: (slot(j, BELOW, *upper), slot(j, ACROSS, *upper), above),
            TO_ACROSS_DOWN: (slot(j, ABOVE, *lower), slot(j, ACROSS, *lower), below),
            TO_FAR: (slot(j, OWN), slot(j, FAR), far),
            TO_FAR_ABOVE: (slot(j, FAR), slot(j, FAR_BELOW), above),
            TO_FAR_BELOW: (slot(j, FAR), slot(j, FAR_ABOVE), below),
            TO_FAR_ACROSS_UP: (slot(j, FAR_BELOW, *upper), slot(j, FAR_ACROSS, *upper), above),
            TO_FAR_ACROSS_DOWN: (slot(j, FAR_ABOVE, *lower), slot(j, FAR_ACROSS, *lower), below),
        }[kind]
        return copy(kind, j, start, end, device)

    def result(j):
        return pltpu.make_async_copy(
            out.at[j], target.at[:, pl.ds(pl.multiple_of(j * WIDTH, WIDTH), WIDTH)], out_sem.at[j]
        )

    def dot(a, b):
        return jnp.dot(a, b, preferred_element_type=jnp.float32).astype(jnp.bfloat16)

    def encode(j):
        load_sources(j).wait()
        pairs[0, j, 0:K] = dot(enc_t[...], src[j])
        exchange(0, j).start()

    def section(bit, j):
        pl.when(j == 0)(lambda: ready(f"section{bit}"))
        exchange(bit, j).wait_recv()
        mixed = dot(pair_w[bit], pairs[bit, j])
        if bit + 1 < SECTIONS:
            pairs[bit + 1, j, 0:K] = mixed
            exchange(bit + 1, j).start()
        else:
            gathered[j, 0:K] = mixed
            for kind in (TO_FAR, TO_ABOVE, TO_BELOW):
                gather(kind, j).start()

    def relay(j):
        gather(TO_ABOVE, j).wait_recv()
        gather(TO_ACROSS_UP, j).start()
        gather(TO_BELOW, j).wait_recv()
        gather(TO_ACROSS_DOWN, j).start()

    def spread(j):
        gather(TO_FAR, j).wait_recv()
        gather(TO_FAR_ABOVE, j).start()
        gather(TO_FAR_BELOW, j).start()

    def relay_far(j):
        gather(TO_FAR_ABOVE, j).wait_recv()
        gather(TO_FAR_ACROSS_UP, j).start()
        gather(TO_FAR_BELOW, j).wait_recv()
        gather(TO_FAR_ACROSS_DOWN, j).start()

    def finish(j):
        @pl.when(j == 0)
        def _():
            ready("cross")
            ready("local")
            ready("decoder")

        for kind in (TO_ACROSS_UP, TO_ACROSS_DOWN, TO_FAR_ACROSS_UP, TO_FAR_ACROSS_DOWN):
            gather(kind, j).wait_recv()
        blocks[0, 0:K] = dot(cross_w[...], gathered[j])
        offset = 0
        for level in range(LOCAL):
            for parent in range(2**level):
                rows = slice(2 * parent * K, 2 * (parent + 1) * K)
                blocks[level + 1, rows] = dot(
                    local_w[offset + rows.start : offset + rows.stop], blocks[level, parent * K : (parent + 1) * K]
                )
            offset += 2 ** (level + 1) * K
        leaf = dec.shape[0] // 2**LOCAL
        for child in range(2**LOCAL):
            rows = slice(child * leaf, (child + 1) * leaf)
            out[j, rows] = dot(dec[rows], blocks[LOCAL, child * K : (child + 1) * K])
        result(j).start()

    tasks = {"encode": encode, "relay": relay, "spread": spread, "relay_far": relay_far, "finish": finish}
    for bit in range(SECTIONS):
        tasks[f"section{bit}"] = lambda j, bit=bit: section(bit, j)
    body = sorted(TIMES, key=lambda name: TIMES[name] % 1)
    last = max(math.floor(time) for time in TIMES.values())

    def step(t, carry):
        for name in body:
            j = t - math.floor(TIMES[name])
            pl.when((j >= 0) & (j < chunks))(lambda name=name, j=j: tasks[name](j))
        return carry

    lax.fori_loop(0, chunks + last, step, 0)

    def drain(j, carry):
        for bit in range(SECTIONS):
            exchange(bit, j).wait_send()
        for kind in range(SECTIONS, COPIES):
            gather(kind, j).wait_send()
        result(j).wait()
        return carry

    lax.fori_loop(0, chunks, drain, 0)


def shards(sources, encoder, section_weight, cross_weight, local_weight, decoder):
    points, columns = sources.shape
    chunks = columns // WIDTH
    matrices = local_weight.shape[1]
    bf16 = jnp.bfloat16
    anywhere = pl.BlockSpec(memory_space=pl.ANY)
    dma = pltpu.SemaphoreType.DMA
    return pl.pallas_call(
        kernel,
        out_shape=jax.ShapeDtypeStruct((decoder.shape[0], columns), bf16),
        in_specs=[anywhere] * 6,
        out_specs=anywhere,
        scratch_shapes=[
            pltpu.VMEM((chunks, points, WIDTH), bf16),
            pltpu.VMEM((points, K), bf16),
            pltpu.VMEM((K, points), bf16),
            pltpu.VMEM((SECTIONS, K, 2 * K), bf16),
            pltpu.VMEM((K, GROUPS * K), bf16),
            pltpu.VMEM((matrices * K, K), bf16),
            pltpu.VMEM(decoder.shape, bf16),
            pltpu.VMEM((SECTIONS, chunks, 2 * K, WIDTH), bf16),
            pltpu.VMEM((chunks, GROUPS * K, WIDTH), bf16),
            pltpu.VMEM((LOCAL + 1, 2**LOCAL * K, WIDTH), bf16),
            pltpu.VMEM((chunks, decoder.shape[0], WIDTH), bf16),
            dma((1 + 2 * SECTIONS + GROUPS + 2,)),
            dma((chunks,)),
            dma((chunks,)),
            dma((COPIES, chunks)),
            dma((COPIES, chunks)),
        ],
        compiler_params=pltpu.CompilerParams(
            collective_id=0, has_side_effects=True, vmem_limit_bytes=48 * 2**20
        ),
        name="butterfly",
    )(sources, encoder, section_weight, cross_weight, local_weight.reshape(1, matrices * K, K), decoder)


def solution(mesh):
    whole = ("grp", "dev")
    placed = (
        P(whole, None),
        P(whole, None),
        P(whole, None, None, None, None),
        P("grp", "dev", None, None, None),
        P(whole, None, None, None),
        P(whole, None),
    )
    return jax.shard_map(shards, mesh=mesh, in_specs=placed, out_specs=P(whole, None), check_vma=False)
```

```python
import math

import jax
import jax.numpy as jnp
from jax import lax
from jax.experimental import pallas as pl
from jax.experimental.pallas import tpu as pltpu
from jax.sharding import PartitionSpec as P

K = 256
LOCAL = 3
SECTIONS = 5
WIDTH = 128
HELD = 3
MESH = pl.DeviceIdType.MESH

TIMES = {
    "encode": 0.0,
    "section0": 0.45,
    "section1": 1.6,
    "section2": 3.4,
    "section3": 4.5,
    "section4": 5.7,
    "release": 8.41,
    "spread": 10.2,
    "mix": 12.3,
    "finish": 14.4,
}

OWN, PAIR, FAR, FAR_PAIR = range(4)
NEAR = 4
TO_PAIR, TO_FAR, FAR_TO_PAIR, PARTIAL = range(SECTIONS, SECTIONS + 4)
COPIES = SECTIONS + 4


def flip(index, bit):
    size = 2**bit
    return index + size - 2 * size * lax.rem(lax.div(index, size), 2)


def kernel(sources, encoder, section_weight, cross_weight, local_weight, leaves,
           src, enc, enc_t, pair_w, cross_w, local_w, pairs, gathered, sums, partial, blocks,
           load_sem, src_sem, out_sem, send_sem, recv_sem, give_sem, take_sem):
    chunks = src.shape[0]
    grp, dev = lax.axis_index("grp"), lax.axis_index("dev")
    height = lax.div(grp, 2)
    half = lax.rem(grp, 2)

    heights = [height + 1 - 2 * lax.rem(height, 2), lax.rem(height + 3 + 2 * lax.rem(height, 2), 4)]
    across = lax.rem(height + 2, 4)
    beside = [2 * place + half for place in heights]

    partners = [(grp, flip(dev, bit)) for bit in range(SECTIONS)]
    far = (grp + 1 - 2 * half, dev)

    barrier = pltpu.get_barrier_semaphore()
    for device in (*partners, (beside[0], dev), (beside[1], dev), far):
        pl.semaphore_signal(barrier, inc=1, device_id=device, device_id_type=MESH)

    def load_sources(j):
        return pltpu.make_async_copy(
            sources.at[:, pl.ds(pl.multiple_of(j * WIDTH, WIDTH), WIDTH)], src.at[j], src_sem.at[j]
        )

    loads = {"encoder": [(encoder, enc)]}
    for bit in range(SECTIONS):
        loads[f"section{bit}"] = [
            (section_weight.at[0, bit, side], pair_w.at[bit, :, pl.ds(side * K, K)]) for side in range(2)
        ]
    def matrix(place, away):
        return cross_weight.at[0, 0, 2 * place + (1 - half if away else half)]

    def columns(slot):
        return pl.ds(slot * K, K)

    loads["cross"], gifts = [], []
    for turn in range(2):
        for slot, place in ((OWN, height), (PAIR, heights[turn]), (FAR, height), (FAR_PAIR, heights[turn])):
            loads["cross"].append((matrix(place, slot >= FAR), cross_w.at[turn, pl.ds(0, K), columns(slot)]))
        for slot, place in ((OWN, heights[1 - turn]), (PAIR, across), (FAR, heights[1 - turn]), (FAR_PAIR, across)):
            gifts.append(pltpu.make_async_remote_copy(
                src_ref=matrix(place, slot >= FAR), dst_ref=cross_w.at[turn, pl.ds(K, K), columns(slot)],
                send_sem=give_sem.at[turn, slot], recv_sem=take_sem.at[turn, slot],
                device_id=(beside[1 - turn], dev), device_id_type=MESH,
            ))
    loads["local"] = [(local_weight.at[0], local_w)]
    copies, number = {}, 0
    for name, moves in loads.items():
        copies[name] = []
        for start, end in moves:
            copies[name].append(pltpu.make_async_copy(start, end, load_sem.at[number]))
            number += 1

    def begin(name):
        for copy in copies[name]:
            copy.start()

    def ready(name):
        for copy in copies[name]:
            copy.wait()

    begin("encoder")
    load_sources(0).start()
    ready("encoder")
    for block in range(enc.shape[0] // K):
        rows = pl.ds(block * K, K)
        enc_t[:, rows] = enc[rows, :].T
    load_sources(0).wait()
    begin("section0")
    load_sources(1).start()
    begin("section1")
    for j in range(2, chunks):
        load_sources(j).start()
    for bit in range(2, SECTIONS):
        begin(f"section{bit}")
    begin("cross")
    begin("local")
    pl.semaphore_wait(barrier, 8)
    for gift in gifts:
        gift.start()

    def copy(kind, j, start, end, device):
        return pltpu.make_async_remote_copy(
            src_ref=start, dst_ref=end, send_sem=send_sem.at[kind, j], recv_sem=recv_sem.at[kind, j],
            device_id=device, device_id_type=MESH,
        )

    def slot(j, number):
        return gathered.at[j, pl.ds(number * K, K)]

    def exchange(bit, j):
        return copy(bit, j, pairs.at[bit, j, pl.ds(0, K)], pairs.at[bit, j, pl.ds(K, K)], partners[bit])

    def gather(kind, j):
        turn = lax.rem(j, 2)
        pair = (beside[0] + turn * (beside[1] - beside[0]), dev)
        other = (beside[1] + turn * (beside[0] - beside[1]), dev)
        start, end, device = {
            TO_PAIR: (slot(j, OWN), slot(j, PAIR), pair),
            TO_FAR: (slot(j, OWN), slot(j, FAR), far),
            FAR_TO_PAIR: (slot(j, FAR), slot(j, FAR_PAIR), pair),
            PARTIAL: (partial.at[0, j], partial.at[1, j], other),
        }[kind]
        return copy(kind, j, start, end, device)

    def result(j):
        return pltpu.make_async_copy(
            blocks.at[j, LOCAL], leaves.at[:, pl.ds(pl.multiple_of(j * WIDTH, WIDTH), WIDTH)], out_sem.at[j]
        )

    def dot32(a, b):
        return jnp.dot(a, b, preferred_element_type=jnp.float32)

    def dot(a, b):
        return dot32(a, b).astype(jnp.bfloat16)

    def encode(j):
        pl.when(j > 0)(lambda: load_sources(j).wait())
        pairs[0, j, 0:K] = dot(enc_t[...], src[j])
        exchange(0, j).start()

    def section(bit, j):
        pl.when(j == 0)(lambda: ready(f"section{bit}"))
        exchange(bit, j).wait_recv()
        mixed = dot(pair_w[bit], pairs[bit, j])
        if bit + 1 < SECTIONS:
            pairs[bit + 1, j, 0:K] = mixed
            exchange(bit + 1, j).start()
        else:
            gathered[j, 0:K] = mixed
            gather(TO_PAIR, j).start()

        if bit + 1 == SECTIONS:
            pl.when(j >= HELD)(lambda: gather(TO_FAR, j).start())

    def release(j):
        @pl.when(j == 0)
        def _():
            for held in range(HELD):
                gather(TO_FAR, held).start()

    def spread(j):
        gather(TO_FAR, j).wait_recv()
        gather(FAR_TO_PAIR, j).start()

    def mix(j):
        @pl.when(j == 0)
        def _():
            ready("cross")
            for gift in gifts:
                gift.wait_recv()

        gather(TO_PAIR, j).wait_recv()
        gather(FAR_TO_PAIR, j).wait_recv()
        both = dot32(cross_w[lax.rem(j, 2)], gathered[j])
        partial[0, j] = both[K:].astype(jnp.bfloat16)
        gather(PARTIAL, j).start()
        sums[j] = both[:K]

    def finish(j):
        @pl.when(j == 0)
        def _():
            ready("local")

        gather(PARTIAL, j).wait_recv()
        blocks[j, 0, 0:K] = (sums[j] + partial[1, j].astype(jnp.float32)).astype(jnp.bfloat16)
        offset = 0
        for level in range(LOCAL):
            for parent in range(2**level):
                rows = slice(2 * parent * K, 2 * (parent + 1) * K)
                blocks[j, level + 1, rows] = dot(
                    local_w[offset + rows.start : offset + rows.stop], blocks[j, level, parent * K : (parent + 1) * K]
                )
            offset += 2 ** (level + 1) * K
        result(j).start()

    tasks = {"encode": encode, "release": release, "spread": spread, "mix": mix, "finish": finish}
    for bit in range(SECTIONS):
        tasks[f"section{bit}"] = lambda j, bit=bit: section(bit, j)
    body = sorted(TIMES, key=lambda name: TIMES[name] % 1)
    last = max(math.floor(time) for time in TIMES.values())

    def step(t, carry):
        for name in body:
            j = t - math.floor(TIMES[name])
            pl.when((j >= 0) & (j < chunks))(lambda name=name, j=j: tasks[name](j))
        return carry

    lax.fori_loop(0, chunks + last, step, 0)

    def drain(j, carry):
        for bit in range(SECTIONS):
            exchange(bit, j).wait_send()
        for kind in range(SECTIONS, COPIES):
            gather(kind, j).wait_send()
        result(j).wait()
        return carry

    lax.fori_loop(0, chunks, drain, 0)
    for gift in gifts:
        gift.wait_send()


def decode(decoder, leaves, target, dec, leaf, out, dec_sem, leaf_sem, out_sem):
    count, rows, _ = dec.shape
    moves = []
    for c in range(count):
        span = pl.ds(c * rows, rows)
        moves.append((
            pltpu.make_async_copy(decoder.at[span], dec.at[c], dec_sem.at[c]),
            pltpu.make_async_copy(leaves.at[pl.ds(c * K, K)], leaf.at[c], leaf_sem.at[c]),
            pltpu.make_async_copy(out.at[c], target.at[span], out_sem.at[c]),
        ))
    for matrix, block, _ in moves:
        matrix.start()
        block.start()
    for c, (matrix, block, result) in enumerate(moves):
        matrix.wait()
        block.wait()
        out[c] = jnp.dot(dec[c], leaf[c], preferred_element_type=jnp.float32).astype(jnp.bfloat16)
        result.start()
    for *_, result in moves:
        result.wait()


def shards(sources, encoder, section_weight, cross_weight, local_weight, decoder):
    points, columns = sources.shape
    chunks = columns // WIDTH
    matrices = local_weight.shape[1]
    bf16 = jnp.bfloat16
    anywhere = pl.BlockSpec(memory_space=pl.ANY)
    dma = pltpu.SemaphoreType.DMA
    leaves = pl.pallas_call(
        kernel,
        out_shape=jax.ShapeDtypeStruct((2**LOCAL * K, columns), bf16),
        in_specs=[anywhere] * 5,
        out_specs=anywhere,
        scratch_shapes=[
            pltpu.VMEM((chunks, points, WIDTH), bf16),
            pltpu.VMEM((points, K), bf16),
            pltpu.VMEM((K, points), bf16),
            pltpu.VMEM((SECTIONS, K, 2 * K), bf16),
            pltpu.VMEM((2, 2 * K, NEAR * K), bf16),
            pltpu.VMEM((matrices * K, K), bf16),
            pltpu.VMEM((SECTIONS, chunks, 2 * K, WIDTH), bf16),
            pltpu.VMEM((chunks, NEAR * K, WIDTH), bf16),
            pltpu.VMEM((chunks, K, WIDTH), jnp.float32),
            pltpu.VMEM((2, chunks, K, WIDTH), bf16),
            pltpu.VMEM((chunks, LOCAL + 1, 2**LOCAL * K, WIDTH), bf16),
            dma((1 + 2 * SECTIONS + 2 * NEAR + 1,)),
            dma((chunks,)),
            dma((chunks,)),
            dma((COPIES, chunks)),
            dma((COPIES, chunks)),
            dma((2, NEAR)),
            dma((2, NEAR)),
        ],
        compiler_params=pltpu.CompilerParams(
            collective_id=0, has_side_effects=True, vmem_limit_bytes=62 * 2**20
        ),
        name="butterfly",
    )(sources, encoder, section_weight, cross_weight, local_weight.reshape(1, matrices * K, K))
    count = 2**LOCAL
    rows = decoder.shape[0] // count
    return pl.pallas_call(
        decode,
        out_shape=jax.ShapeDtypeStruct((decoder.shape[0], columns), bf16),
        in_specs=[anywhere] * 2,
        out_specs=anywhere,
        scratch_shapes=[
            pltpu.VMEM((count, rows, K), bf16),
            pltpu.VMEM((count, K, columns), bf16),
            pltpu.VMEM((count, rows, columns), bf16),
            dma((count,)),
            dma((count,)),
            dma((count,)),
        ],
        compiler_params=pltpu.CompilerParams(vmem_limit_bytes=62 * 2**20),
        name="decode",
    )(decoder, leaves)


def solution(mesh):
    whole = ("grp", "dev")
    placed = (
        P(whole, None),
        P(whole, None),
        P(whole, None, None, None, None),
        P("grp", "dev", None, None, None),
        P(whole, None, None, None),
        P(whole, None),
    )
    return jax.shard_map(shards, mesh=mesh, in_specs=placed, out_specs=P(whole, None), check_vma=False)
```

```python
import math

import jax
import jax.numpy as jnp
from jax import lax
from jax.experimental import pallas as pl
from jax.experimental.pallas import tpu as pltpu
from jax.sharding import PartitionSpec as P

K = 256
LOCAL = 3
SECTIONS = 5
WIDTH = 128
HELD = 3
MESH = pl.DeviceIdType.MESH

TIMES = {
    "encode": 0.0,
    "section0": 0.45,
    "section1": 1.6,
    "section2": 3.4,
    "section3": 4.5,
    "section4": 5.7,
    "release": 8.41,
    "spread": 10.2,
    "mix": 12.3,
    "finish": 14.4,
}

OWN, PAIR, FAR, FAR_PAIR = range(4)
NEAR = 4
TO_PAIR, TO_FAR, FAR_TO_PAIR, PARTIAL = range(SECTIONS, SECTIONS + 4)
COPIES = SECTIONS + 4


def flip(index, bit):
    size = 2**bit
    return index + size - 2 * size * lax.rem(lax.div(index, size), 2)


def kernel(sources, encoder, section_weight, cross_weight, local_weight, decoder, leaves,
           src, enc, enc_t, pair_w, cross_w, local_w, dec, pairs, gathered, sums, partial, blocks,
           load_sem, src_sem, out_sem, send_sem, recv_sem, give_sem, take_sem):
    chunks = src.shape[0]
    grp, dev = lax.axis_index("grp"), lax.axis_index("dev")
    height = lax.div(grp, 2)
    half = lax.rem(grp, 2)

    heights = [height + 1 - 2 * lax.rem(height, 2), lax.rem(height + 3 + 2 * lax.rem(height, 2), 4)]
    across = lax.rem(height + 2, 4)
    beside = [2 * place + half for place in heights]

    partners = [(grp, flip(dev, bit)) for bit in range(SECTIONS)]
    far = (grp + 1 - 2 * half, dev)

    barrier = pltpu.get_barrier_semaphore()
    for device in (*partners, (beside[0], dev), (beside[1], dev), far):
        pl.semaphore_signal(barrier, inc=1, device_id=device, device_id_type=MESH)

    def load_sources(j):
        return pltpu.make_async_copy(
            sources.at[:, pl.ds(pl.multiple_of(j * WIDTH, WIDTH), WIDTH)], src.at[j], src_sem.at[j]
        )

    loads = {"encoder": [(encoder, enc)]}
    for bit in range(SECTIONS):
        loads[f"section{bit}"] = [
            (section_weight.at[0, bit, side], pair_w.at[bit, :, pl.ds(side * K, K)]) for side in range(2)
        ]
    def matrix(place, away):
        return cross_weight.at[0, 0, 2 * place + (1 - half if away else half)]

    def columns(slot):
        return pl.ds(slot * K, K)

    loads["cross"], gifts = [], []
    for turn in range(2):
        for slot, place in ((OWN, height), (PAIR, heights[turn]), (FAR, height), (FAR_PAIR, heights[turn])):
            loads["cross"].append((matrix(place, slot >= FAR), cross_w.at[turn, pl.ds(0, K), columns(slot)]))
        for slot, place in ((OWN, heights[1 - turn]), (PAIR, across), (FAR, heights[1 - turn]), (FAR_PAIR, across)):
            gifts.append(pltpu.make_async_remote_copy(
                src_ref=matrix(place, slot >= FAR), dst_ref=cross_w.at[turn, pl.ds(K, K), columns(slot)],
                send_sem=give_sem.at[turn, slot], recv_sem=take_sem.at[turn, slot],
                device_id=(beside[1 - turn], dev), device_id_type=MESH,
            ))
    loads["local"] = [(local_weight.at[0], local_w)]
    loads["decoder"] = [(decoder, dec)]
    copies, number = {}, 0
    for name, moves in loads.items():
        copies[name] = []
        for start, end in moves:
            copies[name].append(pltpu.make_async_copy(start, end, load_sem.at[number]))
            number += 1

    def begin(name):
        for copy in copies[name]:
            copy.start()

    def ready(name):
        for copy in copies[name]:
            copy.wait()

    begin("encoder")
    load_sources(0).start()
    ready("encoder")
    for block in range(enc.shape[0] // K):
        rows = pl.ds(block * K, K)
        enc_t[:, rows] = enc[rows, :].T
    load_sources(0).wait()
    begin("section0")
    load_sources(1).start()
    begin("section1")
    for j in range(2, chunks):
        load_sources(j).start()
    for bit in range(2, SECTIONS):
        begin(f"section{bit}")
    begin("cross")
    begin("local")
    begin("decoder")
    pl.semaphore_wait(barrier, 8)
    for gift in gifts:
        gift.start()

    def copy(kind, j, start, end, device):
        return pltpu.make_async_remote_copy(
            src_ref=start, dst_ref=end, send_sem=send_sem.at[kind, j], recv_sem=recv_sem.at[kind, j],
            device_id=device, device_id_type=MESH,
        )

    def slot(j, number):
        return gathered.at[j, pl.ds(number * K, K)]

    def exchange(bit, j):
        return copy(bit, j, pairs.at[bit, j, pl.ds(0, K)], pairs.at[bit, j, pl.ds(K, K)], partners[bit])

    def gather(kind, j):
        turn = lax.rem(j, 2)
        pair = (beside[0] + turn * (beside[1] - beside[0]), dev)
        other = (beside[1] + turn * (beside[0] - beside[1]), dev)
        start, end, device = {
            TO_PAIR: (slot(j, OWN), slot(j, PAIR), pair),
            TO_FAR: (slot(j, OWN), slot(j, FAR), far),
            FAR_TO_PAIR: (slot(j, FAR), slot(j, FAR_PAIR), pair),
            PARTIAL: (partial.at[0, j], partial.at[1, j], other),
        }[kind]
        return copy(kind, j, start, end, device)

    def result(j):
        return pltpu.make_async_copy(
            blocks.at[j, LOCAL + 1 - lax.div(j, chunks - 1)], leaves.at[:, pl.ds(pl.multiple_of(j * WIDTH, WIDTH), WIDTH)], out_sem.at[j]
        )

    def dot32(a, b):
        return jnp.dot(a, b, preferred_element_type=jnp.float32)

    def dot(a, b):
        return dot32(a, b).astype(jnp.bfloat16)

    def encode(j):
        pl.when(j > 0)(lambda: load_sources(j).wait())
        pairs[0, j, 0:K] = dot(enc_t[...], src[j])
        exchange(0, j).start()

    def section(bit, j):
        pl.when(j == 0)(lambda: ready(f"section{bit}"))
        exchange(bit, j).wait_recv()
        mixed = dot(pair_w[bit], pairs[bit, j])
        if bit + 1 < SECTIONS:
            pairs[bit + 1, j, 0:K] = mixed
            exchange(bit + 1, j).start()
        else:
            gathered[j, 0:K] = mixed
            gather(TO_PAIR, j).start()

        if bit + 1 == SECTIONS:
            pl.when(j >= HELD)(lambda: gather(TO_FAR, j).start())

    def release(j):
        @pl.when(j == 0)
        def _():
            for held in range(HELD):
                gather(TO_FAR, held).start()

    def spread(j):
        gather(TO_FAR, j).wait_recv()
        gather(FAR_TO_PAIR, j).start()

    def mix(j):
        @pl.when(j == 0)
        def _():
            ready("cross")
            for gift in gifts:
                gift.wait_recv()

        gather(TO_PAIR, j).wait_recv()
        gather(FAR_TO_PAIR, j).wait_recv()
        both = dot32(cross_w[lax.rem(j, 2)], gathered[j])
        partial[0, j] = both[K:].astype(jnp.bfloat16)
        gather(PARTIAL, j).start()
        sums[j] = both[:K]

    def finish(j):
        @pl.when(j == 0)
        def _():
            ready("local")
            ready("decoder")

        gather(PARTIAL, j).wait_recv()
        blocks[j, 0, 0:K] = (sums[j] + partial[1, j].astype(jnp.float32)).astype(jnp.bfloat16)
        offset = 0
        for level in range(LOCAL):
            for parent in range(2**level):
                rows = slice(2 * parent * K, 2 * (parent + 1) * K)
                blocks[j, level + 1, rows] = dot(
                    local_w[offset + rows.start : offset + rows.stop], blocks[j, level, parent * K : (parent + 1) * K]
                )
            offset += 2 ** (level + 1) * K

        @pl.when(j < chunks - 1)
        def _():
            leaf = dec.shape[0] // 2**LOCAL
            for child in range(2**LOCAL):
                rows = slice(child * leaf, (child + 1) * leaf)
                blocks[j, LOCAL + 1, rows] = dot(dec[rows], blocks[j, LOCAL, child * K : (child + 1) * K])

        result(j).start()

    tasks = {"encode": encode, "release": release, "spread": spread, "mix": mix, "finish": finish}
    for bit in range(SECTIONS):
        tasks[f"section{bit}"] = lambda j, bit=bit: section(bit, j)
    body = sorted(TIMES, key=lambda name: TIMES[name] % 1)
    last = max(math.floor(time) for time in TIMES.values())

    def step(t, carry):
        for name in body:
            j = t - math.floor(TIMES[name])
            pl.when((j >= 0) & (j < chunks))(lambda name=name, j=j: tasks[name](j))
        return carry

    lax.fori_loop(0, chunks + last, step, 0)

    def drain(j, carry):
        for bit in range(SECTIONS):
            exchange(bit, j).wait_send()
        for kind in range(SECTIONS, COPIES):
            gather(kind, j).wait_send()
        result(j).wait()
        return carry

    lax.fori_loop(0, chunks, drain, 0)
    for gift in gifts:
        gift.wait_send()


def decode(dec, leaves, target, leaf, leaf_sem, out_sem):
    count, rows, columns = leaf.shape
    last = pl.ds(columns - WIDTH, WIDTH)
    moves = []
    for c in range(count):
        span = pl.ds(c * rows, rows)
        moves.append((
            pltpu.make_async_copy(leaves.at[span], leaf.at[c], leaf_sem.at[c]),
            pltpu.make_async_copy(leaf.at[c], target.at[span], out_sem.at[c]),
        ))
    for block, _ in moves:
        block.start()
    for c, (block, result) in enumerate(moves):
        block.wait()
        leaf[c, :, last] = jnp.dot(
            dec[c * rows : (c + 1) * rows], leaf[c, :, last], preferred_element_type=jnp.float32
        ).astype(jnp.bfloat16)
        result.start()
    for _, result in moves:
        result.wait()


def shards(sources, encoder, section_weight, cross_weight, local_weight, decoder):
    points, columns = sources.shape
    chunks = columns // WIDTH
    matrices = local_weight.shape[1]
    bf16 = jnp.bfloat16
    anywhere = pl.BlockSpec(memory_space=pl.ANY)
    dma = pltpu.SemaphoreType.DMA
    leaves = pl.pallas_call(
        kernel,
        out_shape=jax.ShapeDtypeStruct((2**LOCAL * K, columns), bf16),
        in_specs=[anywhere] * 6,
        out_specs=anywhere,
        scratch_shapes=[
            pltpu.VMEM((chunks, points, WIDTH), bf16),
            pltpu.VMEM((points, K), bf16),
            pltpu.VMEM((K, points), bf16),
            pltpu.VMEM((SECTIONS, K, 2 * K), bf16),
            pltpu.VMEM((2, 2 * K, NEAR * K), bf16),
            pltpu.VMEM((matrices * K, K), bf16),
            pltpu.VMEM(decoder.shape, bf16),
            pltpu.VMEM((SECTIONS, chunks, 2 * K, WIDTH), bf16),
            pltpu.VMEM((chunks, NEAR * K, WIDTH), bf16),
            pltpu.VMEM((chunks, K, WIDTH), jnp.float32),
            pltpu.VMEM((2, chunks, K, WIDTH), bf16),
            pltpu.VMEM((chunks, LOCAL + 2, 2**LOCAL * K, WIDTH), bf16),
            dma((1 + 2 * SECTIONS + 2 * NEAR + 2,)),
            dma((chunks,)),
            dma((chunks,)),
            dma((COPIES, chunks)),
            dma((COPIES, chunks)),
            dma((2, NEAR)),
            dma((2, NEAR)),
        ],
        compiler_params=pltpu.CompilerParams(
            collective_id=0, has_side_effects=True, vmem_limit_bytes=60 * 2**20
        ),
        name="butterfly",
    )(sources, encoder, section_weight, cross_weight, local_weight.reshape(1, matrices * K, K), decoder)
    count = 2**LOCAL
    rows = decoder.shape[0] // count
    assert rows == K
    return pl.pallas_call(
        decode,
        out_shape=jax.ShapeDtypeStruct((decoder.shape[0], columns), bf16),
        in_specs=[pl.BlockSpec(memory_space=pltpu.VMEM), anywhere],
        out_specs=anywhere,
        scratch_shapes=[
            pltpu.VMEM((count, rows, columns), bf16),
            dma((count,)),
            dma((count,)),
        ],
        compiler_params=pltpu.CompilerParams(vmem_limit_bytes=50 * 2**20),
        name="decode",
    )(decoder, leaves)


def solution(mesh):
    whole = ("grp", "dev")
    placed = (
        P(whole, None),
        P(whole, None),
        P(whole, None, None, None, None),
        P("grp", "dev", None, None, None),
        P(whole, None, None, None),
        P(whole, None),
    )
    return jax.shard_map(shards, mesh=mesh, in_specs=placed, out_specs=P(whole, None), check_vma=False)
```
